32 devices in a mesh: task: 4 (over x, core), dp: 8 (over z, y).
Axes of the slice: x: 2, y: 2, z: 4, core: 2. Of those that a mesh axis runs over, the one named last changes fastest.
Arguments:
- inputs: bfloat16 [8192, 4096], P('dp'), may hold values from -6 to 6
- cotangent: bfloat16 [4, 8192, 1024], P('task', 'dp'), may hold values from -0.44194174 to 0.44194174
- task_order: int32 [4], replicated, may hold values from 0 to 3, each once
- conflict_flags: int32 [4, 4], replicated, may hold values 0 or 1
Outputs:
- combined: bfloat16 [4096, 1024], P(None, 'task')
The draws below stay inside these ranges and needn't reach their ends.
Inputs may be any that keep to these rules, and one draw needn't show every extreme that they name: `task_order`: a permutation of the tasks. `conflict_flags`: diagonal entries are ignored.
All inputs are finite; a program needn't handle non-finite values.
Results may differ from the reference program's by a relative error of at most 0.001.
Values may be sent and summed in bfloat16 or wider, within the bound.
A program may use at most 128 MiB of HBM per device.

```python
import math
import jax
import jax.numpy as jnp
from jax import lax

D = 4096
KVW = 1024
TASKS = 4
TOKENS = 8192


def latent_factors(key):
    return jax.random.normal(jax.random.fold_in(key, 21), (TOKENS, 32, 16), jnp.float32)


def draw_inputs(key, part):
    latent = latent_factors(key)
    loading = jax.random.normal(jax.random.fold_in(key, 22), (16, 32, D // 32), jnp.float32) / 4.0
    independent = jax.random.normal(jax.random.fold_in(key, 23), (TOKENS, D), jnp.float32)
    grouped = jnp.einsum('ngr,rgf->ngf', latent, loading).reshape(TOKENS, D)
    values = 0.8 * grouped + 0.6 * independent
    position = jnp.arange(D, dtype=jnp.float32) / (D - 1.0)
    low_end = math.log(0.5)
    high_end = math.log(2.0)
    feature_scale = jnp.exp(low_end + (high_end - low_end) * position)
    values = values * feature_scale[None, :]
    return jnp.clip(values, -6.0, 6.0).astype(jnp.bfloat16)


def draw_cotangent(key, part):
    key_mix = jax.random.fold_in(key, 11)
    key_base = jax.random.fold_in(key, 12)
    key_own = jax.random.fold_in(key, 13)
    key_basis = jax.random.fold_in(key, 15)
    key_signs = jax.random.fold_in(key, 16)
    key_columns = jax.random.fold_in(key, 17)
    key_order = jax.random.fold_in(key, 18)
    key_second = jax.random.fold_in(key, 19)
    key_other = jax.random.fold_in(key, 20)
    sign_values = jnp.where(jax.random.bernoulli(key_order, 0.5, (TASKS,)), 1.0, -1.0).astype(jnp.float32)
    magnitude = jax.random.uniform(key_mix, (TASKS,), jnp.float32, 0.3, 1.0)
    mixing = (sign_values * magnitude)[:, None, None]
    second_mix = jax.random.uniform(key_second, (TASKS, 1, 1), jnp.float32, -1.0, 1.0)
    latent = latent_factors(key)
    basis_rows = jax.random.normal(key_basis, (512, KVW), jnp.float32)
    row_signs = jax.random.uniform(key_signs, (TASKS, 32), jnp.float32, -1.0, 1.0)
    column_scales = jnp.exp(jax.random.uniform(key_columns, (TASKS, 8), jnp.float32, math.log(0.5), math.log(2.0)))
    weighted = (latent[None] * row_signs[:, None, :, None]).reshape(TASKS, TOKENS, 512)
    structured = jnp.einsum('tnk,kc->tnc', weighted, basis_rows)
    structured = structured * jnp.repeat(column_scales, KVW // 8, axis=1)[:, None, :]
    structured = structured * (0.25 / math.sqrt(512.0))
    shared = jnp.clip(jax.random.normal(key_base, (TOKENS, KVW), jnp.float32), -4.0, 4.0)
    other = jnp.clip(jax.random.normal(key_other, (TOKENS, KVW), jnp.float32), -4.0, 4.0)
    private = jnp.clip(jax.random.normal(key_own, (TASKS, TOKENS, KVW), jnp.float32), -4.0, 4.0)
    raw = 0.8 * mixing * shared[None] + second_mix * other[None] + 0.45 * private + structured
    raw = jnp.clip(raw, -4.0, 4.0)
    values = raw / math.sqrt(TOKENS)
    return values.astype(jnp.bfloat16)


def set_ends(values, key, smallest, high):
    index_at = [jax.random.randint(jax.random.fold_in(key, axis), (), 0, length) for axis, length in enumerate(values.shape)]
    main_axis = values.shape.index(max(values.shape))
    beside = index_at[:main_axis] + [(index_at[main_axis] + 1) % values.shape[main_axis]] + index_at[main_axis + 1:]
    return values.at[tuple(index_at)].set(smallest).at[tuple(beside)].set(high)


def setup_inputs(seed: int = 0) -> dict:
    key_of = jax.random.split(jax.random.key(seed), 5)
    inputs = draw_inputs(jax.random.fold_in(key_of[4], 71), 0)
    cotangent = draw_cotangent(jax.random.fold_in(key_of[4], 71), 0)
    task_order = jax.random.permutation(key_of[2], TASKS).astype(jnp.int32)
    conflict_flags = set_ends((jax.random.randint(key_of[3], (TASKS, TASKS), 0, 4) < 3).astype(jnp.int32), jax.random.fold_in(key_of[3], 1), 0, 1)
    return {"inputs": inputs, "cotangent": cotangent, "task_order": task_order, "conflict_flags": conflict_flags}


def project_weights(gram_matrix, task_order, conflict_flags):
    count = gram_matrix.shape[0]
    labels = jnp.arange(count, dtype=jnp.int32)
    coefficients = jnp.eye(count, dtype=jnp.float32)
    for position in range(count):
        target = task_order[position]
        pick_column = (labels == target).astype(jnp.float32)
        column = jnp.dot(gram_matrix, pick_column, precision=lax.Precision.HIGHEST)
        inner_dots = jnp.dot(coefficients, column, precision=lax.Precision.HIGHEST)
        own_square = jnp.sum(pick_column * column)
        active = jnp.dot(conflict_flags.astype(jnp.float32), pick_column, precision=lax.Precision.HIGHEST) * (1.0 - pick_column)
        removed = jnp.minimum(inner_dots, 0.0) / own_square * active
        coefficients = coefficients - removed[:, None] * pick_column[None, :]
    return jnp.sum(coefficients, axis=0)


def reference(inputs, cotangent, task_order, conflict_flags):
    def one_task(task_cot):
        return lax.dot_general(inputs, task_cot, (((0,), (0,)), ((), ())), preferred_element_type=jnp.float32)

    grads = lax.map(one_task, cotangent)
    gram_matrix = jnp.einsum("tab,sab->ts", grads, grads, precision=lax.Precision.HIGHEST)
    weights = project_weights(gram_matrix, task_order, conflict_flags)
    combined = jnp.einsum("t,tab->ab", weights, grads, precision=lax.Precision.HIGHEST)
    return combined.astype(jnp.bfloat16)
```

```python
import functools

import jax
import jax.numpy as jnp
from jax import lax
from jax.experimental import pallas as pl
from jax.experimental.pallas import tpu as pltpu
from jax.sharding import PartitionSpec as P

MESH = pl.DeviceIdType.MESH
TOP = 32767.0


def coded(tile):
    high = jnp.maximum(jnp.max(jnp.abs(tile), axis=0, keepdims=True), 1e-30)
    code = jnp.round(tile * (TOP / high)).astype(jnp.int32).astype(jnp.int16)
    return code, high * (1.0 / TOP)


def decoded(code, scale):
    return code.astype(jnp.int32).astype(jnp.float32) * scale


def kernel(tasks, ndp, chunks, order_ref, flags_ref, x_ref, c_ref, out_ref,
           ysend, yscale, yrecv, yrscale, zsend, zscale, zrecv, zrscale, own,
           gsend, grads, gram_own, gram_dp, gram_mid, gram_task,
           ys_sem, yr_sem, zs_sem, zr_sem, ts_sem, tr_sem, gs_sem, gr_sem,
           hs_sem, hr_sem, as_sem, ar_sem):
    nz = ndp // 2
    me_t = lax.axis_index("task")
    me_d = lax.axis_index("dp")
    z = me_d // 2
    y = me_d % 2
    rows = x_ref.shape[1] // ndp
    step = rows // chunks
    width = c_ref.shape[1] // tasks

    def zof(k):
        return lax.rem(z + k, nz)

    def dp_at(zi, yi):
        return zi * 2 + yi

    partner = (me_t, dp_at(z, 1 - y))

    barrier = pltpu.get_barrier_semaphore()
    for k in range(1, ndp):
        pl.semaphore_signal(barrier, inc=1, device_id=(me_t, lax.rem(me_d + k, ndp)), device_id_type=MESH)
    for k in range(1, tasks):
        pl.semaphore_signal(barrier, inc=1, device_id=(lax.rem(me_t + k, tasks), me_d), device_id_type=MESH)
    pl.semaphore_wait(barrier, ndp + tasks - 2)

    def send(src, dst, s, r, device):
        copy = pltpu.make_async_remote_copy(src_ref=src, dst_ref=dst, send_sem=s, recv_sem=r,
                                            device_id=device, device_id_type=MESH)
        copy.start()
        return copy

    def product(zi, yi, c):
        first = pl.multiple_of(dp_at(zi, yi) * rows + c * step, step)
        return lax.dot_general(x_ref[:, pl.ds(first, step)], c_ref[...], (((0,), (0,)), ((), ())),
                               preferred_element_type=jnp.float32)

    ycopies, zcopies, tcopies = {}, {}, {}
    for c in range(chunks):
        def fill(k, carry, c=c):
            code, scale = coded(product(zof(k), 1 - y, c))
            ysend[c, k] = code
            yscale[c, k] = scale
            return carry
        lax.fori_loop(0, nz, fill, 0)
        ycopies[c] = (send(ysend.at[c], yrecv.at[c], ys_sem.at[c, 0], yr_sem.at[c, 0], partner),
                      send(yscale.at[c], yrscale.at[c], ys_sem.at[c, 1], yr_sem.at[c, 1], partner))

    def second(c):
        for copy in ycopies[c]:
            copy.wait_recv()
        zcopies[c] = []
        for k in [*range(nz - 1, 0, -1), 0]:
            total = product(zof(k), y, c) + decoded(yrecv[c, k], yrscale[c, k])
            if k == 0:
                own[c] = total
            else:
                code, scale = coded(total)
                zsend[c, k] = code
                zscale[c, k] = scale
                peer = (me_t, dp_at(zof(k), y))
                zcopies[c] += [send(zsend.at[c, k], zrecv.at[c, k], zs_sem.at[c, k, 0], zr_sem.at[c, k, 0], peer),
                               send(zscale.at[c, k], zrscale.at[c, k], zs_sem.at[c, k, 1], zr_sem.at[c, k, 1], peer)]

    def third(c):
        for copy in zcopies[c]:
            copy.wait_recv()
        total = own[c]
        for k in range(1, nz):
            total = total + decoded(zrecv[c, k], zrscale[c, k])
        for t in range(tasks):
            gsend[c, t] = total[:, t * width:(t + 1) * width]
        grads[me_t, c] = gsend[c, me_t]
        tcopies[c] = []
        for k in range(1, tasks):
            peer = lax.rem(me_t + k, tasks)
            tcopies[c].append(send(gsend.at[c, peer], grads.at[me_t, c], ts_sem.at[c, k], tr_sem.at[c, k],
                                   (peer, me_d)))

    second(0)
    for c in range(1, chunks):
        second(c)
        third(c - 1)
    third(chunks - 1)

    line = lax.broadcasted_iota(jnp.int32, (8, 128), 0)
    lane = lax.broadcasted_iota(jnp.int32, (8, 128), 1)
    gram = jnp.zeros((8, 128), jnp.float32)
    for c in range(chunks):
        for copy in tcopies[c]:
            copy.wait_recv()
    for s in range(tasks):
        for t in range(s, tasks):
            def add(c, total, s=s, t=t):
                both = grads[s, c] * grads[t, c]
                return total + jnp.sum(both.reshape(step // 8, 8, width), axis=0)
            total = lax.fori_loop(0, chunks, add, jnp.zeros((8, width), jnp.float32))
            value = jnp.sum(jnp.sum(total, axis=0, keepdims=True), axis=1, keepdims=True)
            here = ((line == s) & (lane == t)) | ((line == t) & (lane == s))
            gram = gram + jnp.where(here, value, 0.0)

    def swap(value, buffer_own, buffer, count, s_sem, r_sem, device):
        buffer_own[...] = value
        copies = [send(buffer_own, buffer.at[k], s_sem.at[k], r_sem.at[k], device(k)) for k in range(1, count)]
        for k, copy in enumerate(copies, 1):
            copy.wait_recv()
            value = value + buffer[k]
        for copy in copies:
            copy.wait_send()
        return value

    gram = swap(gram, gram_own, gram_dp, ndp, gs_sem, gr_sem, lambda k: (me_t, lax.rem(me_d + k, ndp)))
    gram = swap(gram, gram_mid, gram_task, tasks, hs_sem, hr_sem, lambda k: (lax.rem(me_t + k, tasks), me_d))

    cols = [jnp.sum(jnp.where(lane == m, gram, 0.0), axis=1, keepdims=True) for m in range(tasks)]
    entry = lambda column, i: jnp.sum(jnp.where(line[:, :1] == i, column, 0.0), axis=0, keepdims=True)
    row = line[:, :1]
    coefficients = [(row == m).astype(jnp.float32) for m in range(tasks)]
    flag_cols = []
    for m in range(tasks):
        column = jnp.zeros((8, 1), jnp.float32)
        for i in range(tasks):
            column = column + jnp.where(row == i, flags_ref[i, m].astype(jnp.float32), 0.0)
        flag_cols.append(column)
    for position in range(tasks):
        target = order_ref[position]
        picks = [jnp.where(target == m, 1.0, 0.0) for m in range(tasks)]
        column = sum(cols[m] * picks[m] for m in range(tasks))
        dots = sum(coefficients[m] * entry(column, m) for m in range(tasks))
        square = sum(entry(column, m) * picks[m] for m in range(tasks))
        active = sum(flag_cols[m] * picks[m] for m in range(tasks)) * jnp.where(row == target, 0.0, 1.0)
        removed = jnp.minimum(dots, 0.0) / square * active
        coefficients = [coefficients[m] - removed * picks[m] for m in range(tasks)]
    weights = [jnp.sum(coefficients[m], axis=0, keepdims=True) for m in range(tasks)]

    def block(d):
        return out_ref.at[pl.ds(pl.multiple_of(d * rows, rows), rows), :]

    for c in range(chunks):
        mixed = sum(weights[t] * grads[t, c] for t in range(tasks))
        out_ref[pl.ds(pl.multiple_of(me_d * rows + c * step, step), step), :] = mixed.astype(jnp.bfloat16)
    mine = block(me_d)
    along = {k: send(mine, mine, as_sem.at[0, k], ar_sem.at[0, k], (me_t, dp_at(zof(k), y)))
             for k in range(1, nz)}
    across = [send(mine, mine, as_sem.at[1, 0], ar_sem.at[1, 0], partner)]
    for k in range(1, nz):
        along[k].wait_recv()
        held = block(dp_at(lax.rem(z + nz - k, nz), y))
        across.append(send(held, held, as_sem.at[1, k], ar_sem.at[1, k], partner))
    for copy in across:
        copy.wait_recv()
    for copy in [*across, *along.values()]:
        copy.wait_send()
    for group in (ycopies, zcopies, tcopies):
        for c in range(chunks):
            for copy in group[c]:
                copy.wait_send()


def solution(mesh):
    tasks, ndp = mesh.shape["task"], mesh.shape["dp"]
    nz = ndp // 2

    def on_device(inputs, cotangent, task_order, conflict_flags):
        cot = cotangent[0]
        rows = inputs.shape[1] // ndp
        step = min(rows, 128)
        chunks = rows // step
        kvw = cot.shape[1]
        width = kvw // tasks
        vmem, dma = pltpu.VMEM, pltpu.SemaphoreType.DMA
        f32, i16 = jnp.float32, jnp.int16
        scratch = [
            vmem((chunks, nz, step, kvw), i16), vmem((chunks, nz, 1, kvw), f32),
            vmem((chunks, nz, step, kvw), i16), vmem((chunks, nz, 1, kvw), f32),
            vmem((chunks, nz, step, kvw), i16), vmem((chunks, nz, 1, kvw), f32),
            vmem((chunks, nz, step, kvw), i16), vmem((chunks, nz, 1, kvw), f32),
            vmem((chunks, step, kvw), f32),
            vmem((chunks, tasks, step, width), f32), vmem((tasks, chunks, step, width), f32),
            vmem((8, 128), f32), vmem((ndp, 8, 128), f32), vmem((8, 128), f32), vmem((tasks, 8, 128), f32),
            dma((chunks, 2)), dma((chunks, 2)), dma((chunks, nz, 2)), dma((chunks, nz, 2)),
            dma((chunks, tasks)), dma((chunks, tasks)), dma((ndp,)), dma((ndp,)),
            dma((tasks,)), dma((tasks,)), dma((2, nz)), dma((2, nz)),
        ]
        smem = pl.BlockSpec(memory_space=pltpu.SMEM)
        whole = pl.BlockSpec(memory_space=pltpu.VMEM)
        return pl.pallas_call(
            functools.partial(kernel, tasks, ndp, chunks),
            out_shape=jax.ShapeDtypeStruct((inputs.shape[1], width), jnp.bfloat16),
            in_specs=[smem, smem, whole, whole],
            out_specs=whole,
            scratch_shapes=scratch,
            compiler_params=pltpu.CompilerParams(collective_id=0, has_side_effects=True,
                                                 vmem_limit_bytes=60 * 1024 * 1024),
        )(task_order, conflict_flags, inputs, cot)

    return jax.shard_map(
        on_device, mesh=mesh,
        in_specs=(P("dp", None), P("task", "dp", None), P(), P()),
        out_specs=P(None, "task"), check_vma=False,
    )
```

```python
import functools

import jax
import jax.numpy as jnp
from jax import lax
from jax.experimental import pallas as pl
from jax.experimental.pallas import tpu as pltpu
from jax.sharding import PartitionSpec as P

MESH = pl.DeviceIdType.MESH
TOP = 32767.0


def coded(tile):
    high = jnp.maximum(jnp.max(jnp.abs(tile), axis=0, keepdims=True), 1e-30)
    code = jnp.round(tile * (TOP / high)).astype(jnp.int32).astype(jnp.int16)
    return code, high * (1.0 / TOP)


def decoded(code, scale):
    return code.astype(jnp.int32).astype(jnp.float32) * scale


def kernel(tasks, ndp, chunks, halves, order_ref, flags_ref, x_ref, c_ref, out_ref,
           ysend, yscale, yrecv, yrscale, zsend, zscale, zrecv, zrscale, own, cots,
           gsend, grads, gram_own, gram_dp, gram_mid, gram_task,
           ys_sem, yr_sem, zs_sem, zr_sem, ts_sem, tr_sem, gs_sem, gr_sem,
           hs_sem, hr_sem, as_sem, ar_sem):
    nz = ndp // 2
    me_t = lax.axis_index("task")
    me_d = lax.axis_index("dp")
    z = me_d // 2
    y = me_d % 2
    rows = x_ref.shape[1] // ndp
    step = rows * halves // chunks
    width = c_ref.shape[1] // tasks
    part = width // halves

    def zof(k):
        return lax.rem(z + k, nz)

    def dp_at(zi, yi):
        return zi * 2 + yi

    partner = (me_t, dp_at(z, 1 - y))

    barrier = pltpu.get_barrier_semaphore()
    for k in range(1, ndp):
        pl.semaphore_signal(barrier, inc=1, device_id=(me_t, lax.rem(me_d + k, ndp)), device_id_type=MESH)
    for k in range(1, tasks):
        pl.semaphore_signal(barrier, inc=1, device_id=(lax.rem(me_t + k, tasks), me_d), device_id_type=MESH)
    pl.semaphore_wait(barrier, ndp + tasks - 2)

    def send(src, dst, s, r, device):
        copy = pltpu.make_async_remote_copy(src_ref=src, dst_ref=dst, send_sem=s, recv_sem=r,
                                            device_id=device, device_id_type=MESH)
        copy.start()
        return copy

    def product(zi, yi, c):
        first = pl.multiple_of(dp_at(zi, yi) * rows + c // halves * step, step)
        return lax.dot_general(x_ref[:, pl.ds(first, step)], cots[c % halves], (((0,), (0,)), ((), ())),
                               preferred_element_type=jnp.float32)

    for h in range(halves):
        for t in range(tasks):
            cots[h, :, t * part:(t + 1) * part] = c_ref[:, t * width + h * part:t * width + (h + 1) * part]

    ycopies, zcopies, tcopies = {}, {}, {}
    for c in range(chunks):
        def fill(k, carry, c=c):
            code, scale = coded(product(zof(k), 1 - y, c))
            ysend[c, k] = code
            yscale[c, k] = scale
            return carry
        lax.fori_loop(0, nz, fill, 0)
        ycopies[c] = (send(ysend.at[c], yrecv.at[c], ys_sem.at[c, 0], yr_sem.at[c, 0], partner),
                      send(yscale.at[c], yrscale.at[c], ys_sem.at[c, 1], yr_sem.at[c, 1], partner))

    def second(c):
        for copy in ycopies[c]:
            copy.wait_recv()
        zcopies[c] = []
        for k in [*range(nz - 1, 0, -1), 0]:
            total = product(zof(k), y, c) + decoded(yrecv[c, k], yrscale[c, k])
            if k == 0:
                own[c] = total
            else:
                code, scale = coded(total)
                zsend[c, k] = code
                zscale[c, k] = scale
                peer = (me_t, dp_at(zof(k), y))
                zcopies[c] += [send(zsend.at[c, k], zrecv.at[c, k], zs_sem.at[c, k, 0], zr_sem.at[c, k, 0], peer),
                               send(zscale.at[c, k], zrscale.at[c, k], zs_sem.at[c, k, 1], zr_sem.at[c, k, 1], peer)]

    def third(c):
        for copy in zcopies[c]:
            copy.wait_recv()
        total = own[c]
        for k in range(1, nz):
            total = total + decoded(zrecv[c, k], zrscale[c, k])
        for t in range(tasks):
            gsend[c, t] = total[:, t * part:(t + 1) * part]
        grads[me_t, c] = gsend[c, me_t]
        tcopies[c] = []
        for k in range(1, tasks):
            peer = lax.rem(me_t + k, tasks)
            tcopies[c].append(send(gsend.at[c, peer], grads.at[me_t, c], ts_sem.at[c, k], tr_sem.at[c, k],
                                   (peer, me_d)))

    pairs = [(s, t) for s in range(tasks) for t in range(s, tasks)]
    sums = {pair: jnp.zeros((8, part), jnp.float32) for pair in pairs}

    def fourth(c):
        for copy in tcopies[c]:
            copy.wait_recv()
        held = [grads[t, c] for t in range(tasks)]
        for s, t in pairs:
            both = held[s] * held[t]
            sums[s, t] = sums[s, t] + jnp.sum(both.reshape(step // 8, 8, part), axis=0)

    for c in range(chunks + 2):
        if c < chunks:
            second(c)
        if 0 <= c - 1 < chunks:
            third(c - 1)
        if c >= 2:
            fourth(c - 2)

    line = lax.broadcasted_iota(jnp.int32, (8, 128), 0)
    lane = lax.broadcasted_iota(jnp.int32, (8, 128), 1)
    gram = jnp.zeros((8, 128), jnp.float32)
    for s, t in pairs:
        value = jnp.sum(jnp.sum(sums[s, t], axis=0, keepdims=True), axis=1, keepdims=True)
        here = ((line == s) & (lane == t)) | ((line == t) & (lane == s))
        gram = gram + jnp.where(here, value, 0.0)

    def swap(value, buffer_own, buffer, count, s_sem, r_sem, device):
        buffer_own[...] = value
        copies = [send(buffer_own, buffer.at[k], s_sem.at[k], r_sem.at[k], device(k)) for k in range(1, count)]
        for k, copy in enumerate(copies, 1):
            copy.wait_recv()
            value = value + buffer[k]
        for copy in copies:
            copy.wait_send()
        return value

    gram = swap(gram, gram_own, gram_dp, ndp, gs_sem, gr_sem, lambda k: (me_t, lax.rem(me_d + k, ndp)))
    gram = swap(gram, gram_mid, gram_task, tasks, hs_sem, hr_sem, lambda k: (lax.rem(me_t + k, tasks), me_d))

    cols = [jnp.sum(jnp.where(lane == m, gram, 0.0), axis=1, keepdims=True) for m in range(tasks)]
    entry = lambda column, i: jnp.sum(jnp.where(line[:, :1] == i, column, 0.0), axis=0, keepdims=True)
    row = line[:, :1]
    coefficients = [(row == m).astype(jnp.float32) for m in range(tasks)]
    flag_cols = []
    for m in range(tasks):
        column = jnp.zeros((8, 1), jnp.float32)
        for i in range(tasks):
            column = column + jnp.where(row == i, flags_ref[i, m].astype(jnp.float32), 0.0)
        flag_cols.append(column)
    for position in range(tasks):
        target = order_ref[position]
        picks = [jnp.where(target == m, 1.0, 0.0) for m in range(tasks)]
        column = sum(cols[m] * picks[m] for m in range(tasks))
        dots = sum(coefficients[m] * entry(column, m) for m in range(tasks))
        square = sum(entry(column, m) * picks[m] for m in range(tasks))
        active = sum(flag_cols[m] * picks[m] for m in range(tasks)) * jnp.where(row == target, 0.0, 1.0)
        removed = jnp.minimum(dots, 0.0) / square * active
        coefficients = [coefficients[m] - removed * picks[m] for m in range(tasks)]
    weights = [jnp.sum(coefficients[m], axis=0, keepdims=True) for m in range(tasks)]

    def block(d):
        return out_ref.at[pl.ds(pl.multiple_of(d * rows, rows), rows), :]

    for c in range(chunks):
        mixed = sum(weights[t] * grads[t, c] for t in range(tasks))
        first = pl.multiple_of(me_d * rows + c // halves * step, step)
        h = c % halves
        out_ref[pl.ds(first, step), h * part:(h + 1) * part] = mixed.astype(jnp.bfloat16)
    mine = block(me_d)
    along = {k: send(mine, mine, as_sem.at[0, k], ar_sem.at[0, k], (me_t, dp_at(zof(k), y)))
             for k in range(1, nz)}
    across = [send(mine, mine, as_sem.at[1, 0], ar_sem.at[1, 0], partner)]
    for k in range(1, nz):
        along[k].wait_recv()
        held = block(dp_at(lax.rem(z + nz - k, nz), y))
        across.append(send(held, held, as_sem.at[1, k], ar_sem.at[1, k], partner))
    for copy in across:
        copy.wait_recv()
    for copy in [*across, *along.values()]:
        copy.wait_send()
    for group in (ycopies, zcopies, tcopies):
        for c in range(chunks):
            for copy in group[c]:
                copy.wait_send()


def solution(mesh):
    tasks, ndp = mesh.shape["task"], mesh.shape["dp"]
    nz = ndp // 2

    def on_device(inputs, cotangent, task_order, conflict_flags):
        cot = cotangent[0]
        rows = inputs.shape[1] // ndp
        step = min(rows, 128)
        width = cot.shape[1] // tasks
        halves = 2 if width % 256 == 0 else 1
        chunks = rows // step * halves
        part = width // halves
        kvw = part * tasks
        vmem, dma = pltpu.VMEM, pltpu.SemaphoreType.DMA
        f32, i16 = jnp.float32, jnp.int16
        scratch = [
            vmem((chunks, nz, step, kvw), i16), vmem((chunks, nz, 1, kvw), f32),
            vmem((chunks, nz, step, kvw), i16), vmem((chunks, nz, 1, kvw), f32),
            vmem((chunks, nz, step, kvw), i16), vmem((chunks, nz, 1, kvw), f32),
            vmem((chunks, nz, step, kvw), i16), vmem((chunks, nz, 1, kvw), f32),
            vmem((chunks, step, kvw), f32), vmem((halves, cot.shape[0], kvw), cot.dtype),
            vmem((chunks, tasks, step, part), f32), vmem((tasks, chunks, step, part), f32),
            vmem((8, 128), f32), vmem((ndp, 8, 128), f32), vmem((8, 128), f32), vmem((tasks, 8, 128), f32),
            dma((chunks, 2)), dma((chunks, 2)), dma((chunks, nz, 2)), dma((chunks, nz, 2)),
            dma((chunks, tasks)), dma((chunks, tasks)), dma((ndp,)), dma((ndp,)),
            dma((tasks,)), dma((tasks,)), dma((2, nz)), dma((2, nz)),
        ]
        smem = pl.BlockSpec(memory_space=pltpu.SMEM)
        whole = pl.BlockSpec(memory_space=pltpu.VMEM)
        return pl.pallas_call(
            functools.partial(kernel, tasks, ndp, chunks, halves),
            out_shape=jax.ShapeDtypeStruct((inputs.shape[1], width), jnp.bfloat16),
            in_specs=[smem, smem, whole, whole],
            out_specs=whole,
            scratch_shapes=scratch,
            compiler_params=pltpu.CompilerParams(collective_id=0, has_side_effects=True,
                                                 vmem_limit_bytes=60 * 1024 * 1024),
        )(task_order, conflict_flags, inputs, cot)

    return jax.shard_map(
        on_device, mesh=mesh,
        in_specs=(P("dp", None), P("task", "dp", None), P(), P()),
        out_specs=P(None, "task"), check_vma=False,
    )
```
